768 devices in a mesh: slab: 192 (over z, y, core), tile: 4 (over x).
Axes of the slice: x: 4, y: 8, z: 12, core: 2. Of those that a mesh axis runs over, the one named last changes fastest.
Arguments:
- load_field: float32 [3072, 16, 256], P(('slab', 'tile')), may hold values from -6 to 6
- orders: int32 [3072], P(('slab', 'tile')), may hold values from 7 to 15
- stiffness: float32 [3072, 768], P(('slab', 'tile')), may hold values from -1 to 5, as said below
- basis_table: float32 [3072, 768], P(('slab', 'tile')), may hold values from -0.25 to 1.25
- eigen_values: float32 [3072, 48], P(('slab', 'tile')), may hold values from 0.3 to 6
- route_plan: int32 [3072], P(('slab', 'tile')), may hold values from 0 to 3071, as said below
Outputs:
- solution: float32 [3072, 16, 256], P(('slab', 'tile'))
- residual: float32 [3072, 16, 256], P(('slab', 'tile'))
The draws below stay inside these ranges and needn't reach their ends.
Inputs may be any that keep to these rules, and one draw needn't show every extreme that they name: `route_plan`: A permutation of all element indices. The element of the device at slab index p and tile index t with value v goes to the device at slab index (p + g) mod the slab axis's size and tile index t, where g = (v mod 4) // 1 is below 4; v = (that device's index) * 4 + (v mod 4). Every device's 4 slots are used, 1 by each of the devices 0 to 3 slab steps behind it. `stiffness`: three symmetric matrices per element with positive diagonals.
All inputs are finite; a program needn't handle non-finite values.
Results may differ from the reference program's by a relative error of at most 0.0003.
Values sent between devices are 32-bit elements; how exact they have to be, the bound alone decides.
No kernel may reach another device: no remote copies, remote signals or barrier semaphores. Data moves between devices by JAX's collectives and lax.ppermute only.
A program may use at most 32 MiB of HBM per device.

```python
import jax
import jax.numpy as jnp
from jax import lax

NB = 16
E_DEV = 4
GROUP = 4
DEG = 2
APPS = 2
ELEMS = 3072
N_SLAB = 192
N_TILE = 4


def plan_table(key):
    devices = N_SLAB * N_TILE
    keys = jax.random.split(jax.random.fold_in(key, 17), devices)
    slot_index = jax.vmap(lambda subkey: jax.random.permutation(subkey, E_DEV))(keys).astype(jnp.int32)
    device = jnp.arange(devices, dtype=jnp.int32)
    slab_index = device // N_TILE
    tile_index = device % N_TILE
    offset = slot_index // (E_DEV // GROUP)
    target = (slab_index[:, None] + offset) % N_SLAB * N_TILE + tile_index[:, None]
    return (target * E_DEV + slot_index).reshape(-1).astype(jnp.int32)


def float_tables(key):
    number = N_SLAB * N_TILE * E_DEV
    route = plan_table(key)
    keys = jax.random.split(jax.random.fold_in(key, 29), 4)
    shape = (number, 3, NB, NB)
    diagonal = jnp.exp(jax.random.uniform(keys[0], (number, 3, NB), jnp.float32, jnp.log(0.5), jnp.log(4.0)))
    factor = jnp.exp(jax.random.uniform(keys[1], (number, 3, NB), jnp.float32, jnp.log(0.7), jnp.log(1.4)))
    noise_stiff = jax.random.truncated_normal(keys[2], -3.0, 3.0, shape, jnp.float32)
    noise_basis = jax.random.truncated_normal(keys[3], -3.0, 3.0, shape, jnp.float32)
    symmetric = 0.5 * (noise_stiff + jnp.swapaxes(noise_stiff, -1, -2))
    root = jnp.sqrt(diagonal)
    identity = jnp.eye(NB, dtype=jnp.float32)
    stiffness = root[..., :, None] * (identity + 0.08 * symmetric) * root[..., None, :]
    basis_home = identity + 0.08 * noise_basis
    eigen_home = diagonal * factor
    basis_table = jnp.zeros((number, 3 * NB * NB), jnp.float32).at[route].set(basis_home.reshape(number, 3 * NB * NB))
    eigen_values = jnp.zeros((number, 3 * NB), jnp.float32).at[route].set(eigen_home.reshape(number, 3 * NB))
    return (stiffness.reshape(number, 3 * NB * NB), basis_table, eigen_values)


def draw_route_plan(key, part):
    return plan_table(key)


def draw_stiffness(key, part):
    return float_tables(key)[0]


def draw_basis_table(key, part):
    return float_tables(key)[1]


def draw_eigen_values(key, part):
    return float_tables(key)[2]


def place_ends(entries, key, smallest, largest):
    index_at = [jax.random.randint(jax.random.fold_in(key, axis), (), 0, length) for axis, length in enumerate(entries.shape)]
    widest = entries.shape.index(max(entries.shape))
    beside = index_at[:widest] + [(index_at[widest] + 1) % entries.shape[widest]] + index_at[widest + 1:]
    return entries.at[tuple(index_at)].set(smallest).at[tuple(beside)].set(largest)


def block_levels(stream_key, extent, cuts, smallest, high):
    gain = 1.0
    for dim, blocks in cuts:
        steps = jax.random.uniform(jax.random.fold_in(jax.random.fold_in(stream_key, 6), dim), (blocks,), jnp.float32, smallest / len(cuts), high / len(cuts))
        gain = gain * jnp.repeat(jnp.exp(steps), extent[dim] // blocks).reshape((-1,) + (1,) * (len(extent) - 1 - dim))
    return gain


def gaussian(own_key, shape, scale, most, cuts=(), held_as=jnp.bfloat16):
    factor_of = block_levels(own_key, shape, cuts, -0.22, 0.18) if cuts else 1.0
    entries = jax.random.normal(own_key, shape, jnp.float32) * scale * factor_of
    return jnp.minimum(jnp.maximum(entries, -most), most).astype(held_as)


def setup_inputs(seed: int = 0) -> dict:
    key_of = jax.random.split(jax.random.key(seed), 7)
    load_field = gaussian(key_of[0], (ELEMS, NB, NB * NB), 1.0, 6.0, ((0, 768),), jnp.float32)
    orders = place_ends(jax.random.randint(key_of[1], (ELEMS,), NB // 2 - 1, NB), jax.random.fold_in(key_of[1], 1), NB // 2 - 1, NB - 1).astype(jnp.int32)
    stiffness = draw_stiffness(jax.random.fold_in(key_of[6], 71), 0)
    basis_table = draw_basis_table(jax.random.fold_in(key_of[6], 71), 0)
    eigen_values = draw_eigen_values(jax.random.fold_in(key_of[6], 71), 0)
    route_plan = draw_route_plan(jax.random.fold_in(key_of[6], 71), 0)
    return dict(load_field=load_field, orders=orders, stiffness=stiffness, basis_table=basis_table, eigen_values=eigen_values, route_plan=route_plan)


highest = lax.Precision.HIGHEST
cheb_low = 0.4
cheb_high = 8.0


def active_cells(orders, edge_size):
    index = jnp.arange(edge_size, dtype=jnp.int32)
    along = ((index[None, :] < orders[:, None]) | (index[None, :] == edge_size - 1)).astype(jnp.float32)
    plane_mask = (along[:, :, None] * along[:, None, :]).reshape(orders.shape[0], edge_size * edge_size)
    return along[:, :, None] * plane_mask[:, None, :]


def rotate(boxes):
    number, edge_size, plane_size = boxes.shape
    return boxes.reshape(number, edge_size, edge_size, edge_size).transpose(0, 2, 3, 1).reshape(number, edge_size, plane_size)


def prepare_inverse(basis, eigen, edge_size):
    number = basis.shape[0]
    matrices = basis.reshape(number, 3, edge_size, edge_size)
    values = eigen.reshape(number, 3, edge_size)
    cross_sum = (values[:, 1][:, :, None] + values[:, 2][:, None, :]).reshape(number, 1, edge_size * edge_size)
    denominator = values[:, 0][:, :, None] + cross_sum
    return matrices, denominator


def solve_local(boxes, matrices, denominator):
    spectral = boxes
    for direction in range(3):
        spectral = rotate(jnp.einsum('eai,eaq->eiq', matrices[:, direction], spectral, precision=highest))
    spectral = spectral / denominator
    for direction in range(3):
        spectral = rotate(jnp.einsum('eai,eiq->eaq', matrices[:, direction], spectral, precision=highest))
    return spectral


def prepare_stiffness(stiffness, edge_size):
    number = stiffness.shape[0]
    return stiffness.reshape(number, 3, edge_size, edge_size)


def local_operator(vector, matrices):
    total = jnp.einsum('eai,eiq->eaq', matrices[:, 0], vector, precision=highest)
    moved = vector
    for direction in range(1, 3):
        moved = rotate(moved)
        total = rotate(total) + jnp.einsum('eai,eiq->eaq', matrices[:, direction], moved, precision=highest)
    return rotate(total)


def inverse_block(boxes, basis, eigen):
    matrices, denominator = prepare_inverse(basis, eigen, NB)
    return solve_local(boxes, matrices, denominator)


def stiff_block(vector, stiffness):
    return local_operator(vector, prepare_stiffness(stiffness, NB))


def blockwise(function, arrays):
    devices = N_SLAB * N_TILE
    shaped = tuple(item.reshape((devices, E_DEV) + item.shape[1:]) for item in arrays)
    result = lax.map(lambda items: function(*items), shaped)
    return result.reshape((devices * E_DEV,) + result.shape[2:])


def assemble(values, active):
    plane_size = NB * NB
    shape = values.shape
    chain = values.reshape(N_SLAB, N_TILE, E_DEV, NB, plane_size).transpose(1, 0, 2, 3, 4).reshape(N_TILE, N_SLAB * E_DEV, NB, plane_size)
    masks = active.reshape(N_SLAB, N_TILE, E_DEV, NB, plane_size).transpose(1, 0, 2, 3, 4).reshape(N_TILE, N_SLAB * E_DEV, NB, plane_size)
    summed = chain[:, :-1, NB - 1, :] + chain[:, 1:, 0, :]
    chain = chain.at[:, :-1, NB - 1, :].set(summed * masks[:, :-1, NB - 1, :])
    chain = chain.at[:, 1:, 0, :].set(summed * masks[:, 1:, 0, :])
    summed = chain[:-1, :, :, plane_size - NB:] + chain[1:, :, :, :NB]
    chain = chain.at[:-1, :, :, plane_size - NB:].set(summed * masks[:-1, :, :, plane_size - NB:])
    chain = chain.at[1:, :, :, :NB].set(summed * masks[1:, :, :, :NB])
    chain = chain.reshape(N_TILE, N_SLAB, E_DEV, NB, plane_size).transpose(1, 0, 2, 3, 4)
    return chain.reshape(shape)


def reference(load_field, orders, stiffness, basis_table, eigen_values, route_plan):
    active = active_cells(orders, NB)
    shares = assemble(active, active)
    residual = assemble(active * load_field, active)
    weight = active / jnp.maximum(shares, 1.0)
    home_basis = basis_table[route_plan]
    home_eigen = eigen_values[route_plan]

    def precondition(vector):
        solved = blockwise(inverse_block, (weight * vector, home_basis, home_eigen))
        return weight * assemble(active * solved, active)

    def operator_apply(vector):
        image = active * blockwise(stiff_block, (active * vector, stiffness))
        return assemble(image, active)

    center = (cheb_high + cheb_low) / 2.0
    half_range = (cheb_high - cheb_low) / 2.0
    sigma_ratio = center / half_range
    solution = jnp.zeros_like(residual)
    for sweep in range(APPS):
        ratio_now = 1.0 / sigma_ratio
        update = precondition(residual) / center
        solution = solution + update
        residual = residual - operator_apply(update)
        for section in range(1, DEG):
            ratio_next = 1.0 / (2.0 * sigma_ratio - ratio_now)
            update = ratio_next * ratio_now * update + (2.0 * ratio_next / half_range) * precondition(residual)
            solution = solution + update
            residual = residual - operator_apply(update)
            ratio_now = ratio_next
    return solution, residual
```

```python
import jax
import jax.numpy as jnp
from jax import lax
from jax.experimental import pallas as pl
from jax.experimental.pallas import tpu as pltpu
from jax.sharding import PartitionSpec as P

F32 = jnp.float32
BF16 = jnp.bfloat16
NB = 16
PL = 256
CHEB_LOW, CHEB_HIGH = 0.4, 8.0
CENTER = (CHEB_HIGH + CHEB_LOW) / 2.0
HALF = (CHEB_HIGH - CHEB_LOW) / 2.0
SIGMA = CENTER / HALF
RATIO = 1.0 / SIGMA
RATIO_NEXT = 1.0 / (2.0 * SIGMA - RATIO)
STEPS = (
    (0.0, 1.0 / CENTER),
    (RATIO_NEXT * RATIO, 2.0 * RATIO_NEXT / HALF),
) * 2

G_LOAD, G_STIFF, G_BASIS, G_EIG, G_FACE, G_ROWS = 0, 64, 82, 94, 100, 104
C_ACT, C_WGT, C_RD, C_KX, C_FACT, C_GACT, C_FW, C_GW, C_KGG, C_ROWS = (
    0, 256, 512, 768, 896, 904, 912, 920, 928, 936,
)
S_R, S_U, S_X, S_MF, S_GU, S_ROWS = 0, 256, 512, 768, 776, 784


def iota(shape, dim):
    return lax.broadcasted_iota(jnp.int32, shape, dim)


def split(value):
    high = value.astype(BF16)
    low = (value - high.astype(F32)).astype(BF16)
    return high, low


def dot(a, b):
    return jnp.dot(a, b, preferred_element_type=F32)


def blk(n, base=0, size=NB):
    if isinstance(n, int):
        return slice(base + n * size, base + (n + 1) * size)
    return pl.ds(pl.multiple_of(base + n * size, 8), size)


def loop(count, body, unroll):
    def step(i, carry):
        for k in range(unroll):
            body(i * unroll + k)
        return carry

    lax.fori_loop(0, count // unroll, step, 0)


def apply_weights(value, w_ref, n):
    rows = value.shape[0]
    high, low = split(value)
    both = dot(jnp.concatenate([high, low], axis=0), w_ref[blk(2 * n, 0, PL), :])
    return both[:rows] + both[rows:] + dot(high, w_ref[blk(2 * n + 1, 0, PL), :])


def apply_blocks(bd_ref, which, value, t):
    high, low = split(value)
    m_high = bd_ref[which * 512 + t * 64 : which * 512 + (t + 1) * 64, :64]
    m_low = bd_ref[which * 512 + 256 + t * 64 : which * 512 + 256 + (t + 1) * 64, :64]
    both = dot(jnp.concatenate([m_high, m_low], axis=0), high)
    return both[:64] + both[64:] + dot(m_high, low)


def face_stage(value, mask):
    low, high = value[:, :128], value[:, 128:]
    row = iota((8, 128), 0)
    lane = iota((8, 128), 1)
    before = jnp.where(row % 4 == 0, 0.0, pltpu.roll(high, 1, 0))
    after = jnp.where(row % 4 == 3, 0.0, pltpu.roll(low, 7, 0))
    low = low + jnp.where(lane < 16, pltpu.roll(before, 16, 1), 0.0)
    high = high + jnp.where(lane >= 112, pltpu.roll(after, 112, 1), 0.0)
    return jnp.concatenate([low, high], axis=1) * mask


def assemble(v_ref, ext_ref, xp_ref, c_ref, out):
    row = iota((NB, PL), 0)
    lane = iota((NB, 128), 1)

    def x_stage(t):
        for e in range(4):
            n = t * 4 + e
            m = v_ref[blk(n), :]
            if e > 0:
                left = v_ref[pl.ds(n * NB - 1, 1), :]
            else:
                left = ext_ref[pl.ds(t, 1), :]
            if e < 3:
                right = v_ref[pl.ds(n * NB + NB, 1), :]
            else:
                right = ext_ref[pl.ds(4 + t, 1), :]
            total = m + jnp.where(row == 0, left, 0.0) + jnp.where(row == NB - 1, right, 0.0)
            xp_ref[blk(n + 4), :] = total * c_ref[blk(n, C_ACT), :]

    def y_stage(t):
        for e in range(4):
            n = t * 4 + e
            x = xp_ref[blk(n + 4), :]
            before = xp_ref[blk(n), 128:]
            after = xp_ref[blk(n + 8), :128]
            low = x[:, :128] + jnp.where(lane < 16, pltpu.roll(before, 16, 1), 0.0)
            high = x[:, 128:] + jnp.where(lane >= 112, pltpu.roll(after, 112, 1), 0.0)
            z = jnp.concatenate([low, high], axis=1) * c_ref[blk(n, C_ACT), :]
            out(n, z)

    for t in range(4):
        x_stage(t)
    for t in range(4):
        y_stage(t)


def zero_borders(xp_ref):
    xp_ref[0:64, :] = jnp.zeros((64, PL), F32)
    xp_ref[320:384, :] = jnp.zeros((64, PL), F32)


def phase_one(step, c_ref, bd_ref, wf_ref, wb_ref, s_in, s_out, v_ref, v2_ref, xp_ref, ext_ref,
              sm_ref, a_ref, b_ref):
    alpha, beta = step

    def forward(n):
        rows = blk(n)
        value = c_ref[blk(n, C_WGT), :] * s_out[blk(n, S_R), :]
        v2_ref[rows, :] = apply_weights(value, wf_ref, n)

    loop(16, forward, 8)
    for t in range(4):
        h = apply_blocks(bd_ref, 0, v2_ref[t * 64 : t * 64 + 64, :], t)
        h = h * c_ref[C_RD + t * 64 : C_RD + t * 64 + 64, :]
        v2_ref[t * 64 : t * 64 + 64, :] = apply_blocks(bd_ref, 1, h, t)

    def backward(n):
        v_ref[blk(n), :] = c_ref[blk(n, C_ACT), :] * apply_weights(v2_ref[blk(n), :], wb_ref, n)

    loop(16, backward, 8)
    ext_ref[...] = jnp.zeros((8, PL), F32)

    def update(n, z):
        new = beta * (c_ref[blk(n, C_WGT), :] * z)
        if alpha != 0.0:
            new = new + alpha * s_in[blk(n, S_U), :]
        s_out[blk(n, S_U), :] = new

    assemble(v_ref, ext_ref, xp_ref, c_ref, update)
    faces = [v_ref[t * 64 : t * 64 + 1, :] for t in range(4)]
    faces += [v_ref[t * 64 + 63 : t * 64 + 64, :] for t in range(4)]
    faces = jnp.concatenate(faces, axis=0)
    s_out[S_MF : S_MF + 8, :] = faces
    inner = []
    for side in range(2):
        for t in range(4):
            n = t * 4 + 3 * side
            k = c_ref[blk(side * 4 + t, C_KX), :]
            inner.append(jnp.sum(k * s_out[blk(n, S_U), :], axis=0, keepdims=True))
    inner = jnp.concatenate(inner, axis=0)
    to_left = jnp.concatenate([faces[:4], inner[:4]], axis=0)
    to_right = jnp.concatenate([faces[4:], inner[4:]], axis=0)
    even = jnp.full((8, PL), sm_ref[0], jnp.int32) == 0
    a_ref[...] = jnp.where(even, to_right, to_left)
    b_ref[...] = jnp.where(even, to_left, to_right)


def phase_two(step, c_ref, bd_ref, m_ref, s_in, s_out, v_ref, v2_ref, xp_ref, ext_ref, sm_ref,
              a_ref, b_ref):
    alpha, beta = step
    even = jnp.full((8, PL), sm_ref[0], jnp.int32) == 0
    rec_a, rec_b = a_ref[...], b_ref[...]
    from_left = jnp.where(even, rec_b, rec_a)
    from_right = jnp.where(even, rec_a, rec_b)
    outer = jnp.concatenate([from_left[:4], from_right[:4]], axis=0)
    inner = jnp.concatenate([from_left[4:], from_right[4:]], axis=0)
    fact = c_ref[C_FACT : C_FACT + 8, :]
    gact = c_ref[C_GACT : C_GACT + 8, :]
    delta = beta * (c_ref[C_FW : C_FW + 8, :] * face_stage(fact * outer, fact))
    ghost = (outer + s_in[S_MF : S_MF + 8, :]) * gact
    ghost = beta * (c_ref[C_GW : C_GW + 8, :] * face_stage(ghost, gact))
    if alpha != 0.0:
        ghost = ghost + alpha * s_in[S_GU : S_GU + 8, :]
    s_out[S_GU : S_GU + 8, :] = ghost
    row = iota((NB, PL), 0)
    for t in range(4):
        for e in range(4):
            n = t * 4 + e
            u = s_in[blk(n, S_U), :]
            if e == 0:
                u = u + jnp.where(row == 0, delta[t : t + 1], 0.0)
            if e == 3:
                u = u + jnp.where(row == NB - 1, delta[4 + t : 5 + t], 0.0)
            s_out[blk(n, S_U), :] = u
            s_out[blk(n, S_X), :] = s_in[blk(n, S_X), :] + u

    for t in range(4):
        v2_ref[t * 64 : t * 64 + 64, :] = apply_blocks(
            bd_ref, 2, s_out[S_U + t * 64 : S_U + t * 64 + 64, :], t
        )
    high, low = split(ghost)
    both = jnp.concatenate([high, low], axis=0)
    row8 = iota((8, PL), 0)
    image = inner + c_ref[C_KGG : C_KGG + 8, :] * ghost
    for s in range(8):
        w = 16 + s
        part = dot(both, m_ref[blk(2 * w, 0, PL), :])
        part = part[:8] + part[8:] + dot(high, m_ref[blk(2 * w + 1, 0, PL), :])
        image = image + jnp.where(row8 == s, part, 0.0)
    ext_ref[...] = image * gact

    def local(n):
        rows = blk(n)
        q = v2_ref[rows, :] + apply_weights(s_out[blk(n, S_U), :], m_ref, n)
        v_ref[rows, :] = c_ref[blk(n, C_ACT), :] * q

    loop(16, local, 8)

    def update(n, z):
        s_out[blk(n, S_R), :] = s_in[blk(n, S_R), :] - z

    assemble(v_ref, ext_ref, xp_ref, c_ref, update)


def first_kernel(sm_ref, g_ref, c_ref, bd_ref, wf_ref, wb_ref, m_ref, s_ref, a_ref, b_ref,
                 v_ref, v2_ref, xp_ref, ext_ref, p_ref, ta_ref, tb_ref):
    zero_borders(xp_ref)
    row = iota((NB, PL), 0)
    lane = iota((NB, PL), 1)
    by_row = lane // NB == row
    by_col = lane % NB == row
    big_l = iota((PL, PL), 0)
    big_m = iota((PL, PL), 1)

    def hot(condition):
        return jnp.where(condition, 1.0, 0.0).astype(BF16)

    def expand(rows, mask, onehot):
        for i, (t, r) in enumerate(rows):
            p_ref[blk(i), :] = jnp.where(mask, g_ref[t, r : r + 1, :], 0.0)
        size = len(rows) * NB
        for start in range(0, size, 128):
            high, low = split(p_ref[start : start + 128, :])
            yield start, dot(high, onehot) + dot(low, onehot)

    own = [(t, e) for t in range(4) for e in range(4)]
    wide = own + [(t, 4) for t in range(4)] + [(t, 5) for t in range(4)]

    def basis(d):
        return [(t, G_BASIS + 3 * e + d) for t, e in own]

    def stiff(d, which):
        return [(t, G_STIFF + 3 * e + d) for t, e in which]

    e1 = hot(big_l % NB == big_m // NB)
    e2 = hot(big_l % NB == big_m % NB)
    e3 = hot(big_l // NB == big_m // NB)
    e4 = hot(big_l // NB == big_m % NB)
    block = (iota((128, PL), 0) // NB) % 4 == iota((128, PL), 1) // NB
    for which, (rows, mask, onehot) in enumerate(
        ((basis(0), by_col, e4), (basis(0), by_row, e2), (stiff(0, own), by_row, e2))
    ):
        for start, part in expand(rows, mask, onehot):
            high, low = split(jnp.where(block, part, 0.0))
            bd_ref[which * 512 + start : which * 512 + start + 128, :] = high
            bd_ref[which * 512 + 256 + start : which * 512 + 256 + start + 128, :] = low

    eig = jnp.concatenate([g_ref[t, G_EIG + e : G_EIG + e + 1, :] for t, e in wide], axis=0)
    high, low = split(eig)
    orders = dot(high, hot(big_l == 48))
    cross_hot = hot(big_l == 16 + big_m // NB) + hot(big_l == 32 + big_m % NB)
    cross = dot(high, cross_hot) + dot(low, cross_hot)
    for start, part in expand([(t, G_EIG + e) for t, e in own], lane == row, hot(big_l < 16)):
        v_ref[start : start + 128, :] = part
    for n in range(16):
        order = orders[n : n + 1, :]

        def along(index):
            return jnp.where((index.astype(F32) < order) | (index == NB - 1), 1.0, 0.0)

        c_ref[blk(n, C_ACT), :] = along(row) * (along(lane // NB) * along(lane % NB))
        c_ref[blk(n, C_RD), :] = 1.0 / (v_ref[blk(n), :] + cross[n : n + 1, :])
    order = orders[16:24, :]
    lane8 = iota((8, PL), 1)
    row8 = iota((8, PL), 0)

    def along8(index):
        return jnp.where((index.astype(F32) < order) | (index == NB - 1), 1.0, 0.0)

    gact = jnp.where(order > 0.0, along8(lane8 // NB) * along8(lane8 % NB), 0.0)
    fact = jnp.concatenate(
        [c_ref[t * 64 : t * 64 + 1, :] for t in range(4)]
        + [c_ref[t * 64 + 63 : t * 64 + 64, :] for t in range(4)],
        axis=0,
    )
    c_ref[C_FACT : C_FACT + 8, :] = fact
    c_ref[C_GACT : C_GACT + 8, :] = gact
    ghost_shares = face_stage((gact + fact) * gact, gact)
    c_ref[C_GW : C_GW + 8, :] = gact / jnp.maximum(ghost_shares, 1.0)
    for side in range(2):
        for t in range(4):
            e = 3 * side
            kx = g_ref[t, G_STIFF + 3 * e : G_STIFF + 3 * e + 1, :]
            edge = NB - 1 if side else 0
            col = jnp.sum(
                jnp.where((lane == edge * NB + row) & (row != edge), kx, 0.0), axis=1, keepdims=True
            )
            c_ref[blk(side * 4 + t, C_KX), :] = jnp.broadcast_to(col, (NB, PL))
    kgx = jnp.concatenate(
        [g_ref[t, G_STIFF + 12 : G_STIFF + 13, :] for t in range(4)]
        + [g_ref[t, G_STIFF + 15 : G_STIFF + 16, :] for t in range(4)],
        axis=0,
    )
    pick = lane8 == jnp.where(row8 < 4, PL - 1, 0)
    kgg = jnp.sum(jnp.where(pick, kgx, 0.0), axis=1, keepdims=True)
    c_ref[C_KGG : C_KGG + 8, :] = jnp.broadcast_to(kgg, (8, PL))

    v_ref[...] = c_ref[C_ACT : C_ACT + 256, :]
    ext_ref[...] = gact

    def weigh(n, z):
        c_ref[blk(n, C_WGT), :] = c_ref[blk(n, C_ACT), :] / jnp.maximum(z, 1.0)

    assemble(v_ref, ext_ref, xp_ref, c_ref, weigh)
    c_ref[C_FW : C_FW + 8, :] = jnp.concatenate(
        [c_ref[C_WGT + t * 64 : C_WGT + t * 64 + 1, :] for t in range(4)]
        + [c_ref[C_WGT + t * 64 + 63 : C_WGT + t * 64 + 64, :] for t in range(4)],
        axis=0,
    )
    for t in range(4):
        v_ref[t * 64 : t * 64 + 64, :] = c_ref[t * 64 : t * 64 + 64, :] * g_ref[t, 0:64, :]
    ghost_load = jnp.concatenate(
        [g_ref[t, G_FACE : G_FACE + 1, :] for t in range(4)]
        + [g_ref[t, G_FACE + 1 : G_FACE + 2, :] for t in range(4)],
        axis=0,
    )
    ext_ref[...] = gact * ghost_load

    def start_residual(n, z):
        s_ref[blk(n, S_R), :] = z

    assemble(v_ref, ext_ref, xp_ref, c_ref, start_residual)
    s_ref[S_X : S_X + 256, :] = jnp.zeros((256, PL), F32)
    s_ref[S_GU : S_GU + 8, :] = jnp.zeros((8, PL), F32)

    def product(w_ref, mask, rows_y, hot_y, rows_z, hot_z):
        for start, part in expand(rows_y, mask, hot_y):
            ta_ref[start : start + 128, :] = part
        for start, part in expand(rows_z, mask, hot_z):
            tb_ref[start : start + 128, :] = part

        def build(n):
            ty = ta_ref[blk(n), :]
            tz = tb_ref[blk(n), :]
            for b in range(NB):
                high, low = split(ty[b : b + 1, :] * tz)
                w_ref[pl.ds(pl.multiple_of(n * 512 + b * NB, 16), NB), :] = high
                w_ref[pl.ds(pl.multiple_of(n * 512 + 256 + b * NB, 16), NB), :] = low

        loop(16, build, 2)

    product(wf_ref, by_row, basis(1), e1, basis(2), e2)
    product(wb_ref, by_col, basis(1), e3, basis(2), e4)

    for start, part in expand(stiff(1, wide), by_col, e3):
        ta_ref[start : start + 128, :] = part
    for start, part in expand(stiff(2, wide), by_col, e4):
        tb_ref[start : start + 128, :] = part

    def build_sum(n):
        ty = ta_ref[blk(n), :]
        tz = tb_ref[blk(n), :]
        for j in range(NB):
            value = jnp.where(by_col, ty[j : j + 1, :], 0.0)
            value = value + jnp.where(lane // NB == j, tz, 0.0)
            high, low = split(value)
            m_ref[pl.ds(pl.multiple_of(n * 512 + j * NB, 16), NB), :] = high
            m_ref[pl.ds(pl.multiple_of(n * 512 + 256 + j * NB, 16), NB), :] = low

    loop(24, build_sum, 2)
    phase_one(STEPS[0], c_ref, bd_ref, wf_ref, wb_ref, s_ref, s_ref, v_ref, v2_ref, xp_ref,
              ext_ref, sm_ref, a_ref, b_ref)


def middle_kernel(k, sm_ref, ra_ref, rb_ref, c_ref, bd_ref, wf_ref, wb_ref, m_ref, si_ref,
                  so_ref, a_ref, b_ref, v_ref, v2_ref, xp_ref, ext_ref):
    zero_borders(xp_ref)
    phase_two(STEPS[k], c_ref, bd_ref, m_ref, si_ref, so_ref, v_ref, v2_ref, xp_ref, ext_ref,
              sm_ref, ra_ref, rb_ref)
    phase_one(STEPS[k + 1], c_ref, bd_ref, wf_ref, wb_ref, so_ref, so_ref, v_ref, v2_ref, xp_ref,
              ext_ref, sm_ref, a_ref, b_ref)


def last_kernel(sm_ref, ra_ref, rb_ref, c_ref, bd_ref, m_ref, si_ref, x_ref, r_ref,
                so_ref, v_ref, v2_ref, xp_ref, ext_ref):
    zero_borders(xp_ref)
    phase_two(STEPS[3], c_ref, bd_ref, m_ref, si_ref, so_ref, v_ref, v2_ref, xp_ref, ext_ref,
              sm_ref, ra_ref, rb_ref)
    t = sm_ref[1]
    for e in range(4):
        x_ref[e * NB : (e + 1) * NB, :] = so_ref[pl.ds(pl.multiple_of(S_X + t * 64 + e * NB, 8), NB), :]
        r_ref[e * NB : (e + 1) * NB, :] = so_ref[pl.ds(pl.multiple_of(S_R + t * 64 + e * NB, 8), NB), :]


VM = pl.BlockSpec(memory_space=pltpu.VMEM)
SM = pl.BlockSpec(memory_space=pltpu.SMEM)


def struct(rows, dtype=F32):
    return jax.ShapeDtypeStruct((rows, PL), dtype)


WORK = [pltpu.VMEM((256, PL), F32), pltpu.VMEM((256, PL), F32), pltpu.VMEM((384, PL), F32),
        pltpu.VMEM((8, PL), F32)]
LIMIT = pltpu.CompilerParams(vmem_limit_bytes=12 * 2**20)


def call(kernel, name, ins, outs, scratch):
    return pl.pallas_call(
        kernel,
        name=name,
        in_specs=[SM] + [VM] * ins,
        out_specs=[VM] * len(outs),
        out_shape=outs,
        scratch_shapes=scratch,
        compiler_params=LIMIT,
    )


def per_device(load_field, orders, stiffness, basis_table, eigen_values, route_plan):
    slabs = lax.axis_size("slab")
    tiles = lax.axis_size("tile")
    p = lax.axis_index("slab")
    even = p % 2 == 0
    scalars = jnp.stack([p % 2, lax.axis_index("tile")]).astype(jnp.int32)
    swap_a = [(i, i ^ 1) for i in range(slabs)]
    swap_b = [(i, (i + 1) % slabs) if i % 2 else (i, (i - 1) % slabs) for i in range(slabs)]
    swap_in = [(i, j) for i, j in swap_b if abs(i - j) == 1]

    ord_f = orders.astype(F32)
    lane = jnp.arange(PL, dtype=jnp.int32)
    eig_rows = jnp.pad(eigen_values, ((0, 0), (0, PL - eigen_values.shape[1])))
    order_rows = jnp.where(lane[None, :] == 48, ord_f[:, None], 0.0)
    table = basis_table.reshape(4, 3, PL)
    stiff = stiffness.reshape(4, 3, PL)
    slots = jnp.concatenate([table, eig_rows[:, None, :]], axis=1)
    to_right = jnp.concatenate(
        [load_field[3, NB - 1 :, :], stiff[3], order_rows[3:4], jnp.zeros((3, PL), F32)], axis=0
    )
    to_left = jnp.concatenate(
        [load_field[0, :1, :], stiff[0], order_rows[0:1] + eig_rows[1:2], table[1]], axis=0
    )
    rec_a = lax.ppermute(jnp.where(even, to_right, to_left), "slab", swap_a)
    rec_b = lax.ppermute(jnp.where(even, to_left, to_right), "slab", swap_b)
    slot_2 = lax.ppermute(slots[2], "slab", [((i + 2) % slabs, i) for i in range(slabs)])
    slot_3 = lax.ppermute(slots[3], "slab", [((i + 3) % slabs, i) for i in range(slabs)])
    from_right = jnp.where(even, rec_a, rec_b)
    from_left = jnp.where(even, rec_b, rec_a)
    slot_1 = jnp.concatenate(
        [from_right[5:8], jnp.where(lane[None, :] < 48, from_right[4:5], 0.0)], axis=0
    )
    from_left = jnp.where(p == 0, 0.0, from_left)
    from_right = jnp.where(p == slabs - 1, 0.0, from_right)
    which = (route_plan % 4)[:, None, None]
    home = jnp.where(
        which == 0,
        slots[0][None],
        jnp.where(which == 1, slot_1[None], jnp.where(which == 2, slot_2[None], slot_3[None])),
    )
    only_order = lane[None, :] == 48
    block = jnp.concatenate(
        [
            load_field.reshape(64, PL),
            stiff.reshape(12, PL),
            from_left[1:4],
            from_right[1:4],
            home[:, :3].reshape(12, PL),
            home[:, 3] + order_rows,
            jnp.where(only_order, from_left[4:5], 0.0),
            jnp.where(only_order, from_right[4:5], 0.0),
            from_left[0:1],
            from_right[0:1],
            jnp.zeros((2, PL), F32),
        ],
        axis=0,
    )
    gathered = lax.all_to_all(
        jnp.broadcast_to(block[None], (tiles, G_ROWS, PL)), "tile", 0, 0
    )

    state = struct(S_ROWS)
    message = struct(8)
    consts, blocks, w_f, w_b, w_m, s, a, b = call(
        first_kernel,
        "setup_and_solve",
        1,
        [struct(C_ROWS), struct(1536, BF16), struct(16 * 512, BF16), struct(16 * 512, BF16),
         struct(24 * 512, BF16), state, message, message],
        WORK + [pltpu.VMEM((384, PL), F32)] * 3,
    )(scalars, gathered)
    for k in range(3):
        ra = lax.ppermute(a, "slab", swap_a)
        rb = lax.ppermute(b, "slab", swap_in)

        def kernel(*refs, k=k):
            middle_kernel(k, *refs)

        s, a, b = call(kernel, "operator_and_solve_%d" % k, 8, [state, message, message], WORK)(
            scalars, ra, rb, consts, blocks, w_f, w_b, w_m, s
        )
    ra = lax.ppermute(a, "slab", swap_a)
    rb = lax.ppermute(b, "slab", swap_in)
    x, r = call(
        last_kernel, "last_operator", 6, [struct(64), struct(64)],
        [pltpu.VMEM((S_ROWS, PL), F32)] + WORK,
    )(scalars, ra, rb, consts, blocks, w_m, s)
    return x.reshape(load_field.shape), r.reshape(load_field.shape)


def solution(mesh):
    both = ("slab", "tile")
    in_specs = (P(both, None, None), P(both), P(both, None), P(both, None), P(both, None), P(both))
    out_specs = (P(both, None, None), P(both, None, None))
    return jax.shard_map(
        per_device, mesh=mesh, in_specs=in_specs, out_specs=out_specs, check_vma=False
    )
```

```python
import jax
import jax.numpy as jnp
from jax import lax
from jax.experimental import pallas as pl
from jax.experimental.pallas import tpu as pltpu
from jax.sharding import PartitionSpec as P


F32 = jnp.float32
BF16 = jnp.bfloat16
NB = 16
PL = 256
CHEB_LOW, CHEB_HIGH = 0.4, 8.0
CENTER = (CHEB_HIGH + CHEB_LOW) / 2.0
HALF = (CHEB_HIGH - CHEB_LOW) / 2.0
SIGMA = CENTER / HALF
RATIO = 1.0 / SIGMA
RATIO_NEXT = 1.0 / (2.0 * SIGMA - RATIO)
STEPS = (
    (0.0, 1.0 / CENTER),
    (RATIO_NEXT * RATIO, 2.0 * RATIO_NEXT / HALF),
) * 2

G_STIFF, G_TABLE, G_EIG, G_ROWS = 64, 76, 88, 96
F_TABLE, F_EIG, F_FACE, F_STIFF, F_ORDER, F_STEP, F_ROWS = 0, 3, 4, 5, 8, 9, 40
C_ACT, C_KX, C_LOAD, C_SLOT, C_ROWS = 0, 256, 384, 640, 656
D_WGT, D_RD, D_FACT, D_GACT, D_FW, D_GW, D_KGG, D_ROWS = 0, 256, 512, 520, 528, 536, 544, 552
S_R, S_U, S_X, S_MF, S_GU, S_ROWS = 0, 256, 512, 768, 776, 784


def iota(shape, dim):
    return lax.broadcasted_iota(jnp.int32, shape, dim)


def split(value):
    high = value.astype(BF16)
    low = (value - high.astype(F32)).astype(BF16)
    return high, low


def dot(a, b):
    return jnp.dot(a, b, preferred_element_type=F32)


def blk(n, base=0, size=NB):
    if isinstance(n, int):
        return slice(base + n * size, base + (n + 1) * size)
    return pl.ds(pl.multiple_of(base + n * size, 8), size)


def loop(count, body, unroll):
    def step(i, carry):
        for k in range(unroll):
            body(i * unroll + k)
        return carry

    lax.fori_loop(0, count // unroll, step, 0)


def apply_weights(value, w_ref, n):
    rows = value.shape[0]
    high, low = split(value)
    both = dot(jnp.concatenate([high, low], axis=0), w_ref[blk(2 * n, 0, PL), :])
    return both[:rows] + both[rows:] + dot(high, w_ref[blk(2 * n + 1, 0, PL), :])


def apply_blocks(bd_ref, which, value, t):
    high, low = split(value)
    m_high = bd_ref[which * 512 + t * 64 : which * 512 + (t + 1) * 64, :64]
    m_low = bd_ref[which * 512 + 256 + t * 64 : which * 512 + 256 + (t + 1) * 64, :64]
    both = dot(jnp.concatenate([m_high, m_low], axis=0), high)
    return both[:64] + both[64:] + dot(m_high, low)


def face_stage(value, mask):
    low, high = value[:, :128], value[:, 128:]
    row = iota((8, 128), 0)
    lane = iota((8, 128), 1)
    before = jnp.where(row % 4 == 0, 0.0, pltpu.roll(high, 1, 0))
    after = jnp.where(row % 4 == 3, 0.0, pltpu.roll(low, 7, 0))
    low = low + jnp.where(lane < 16, pltpu.roll(before, 16, 1), 0.0)
    high = high + jnp.where(lane >= 112, pltpu.roll(after, 112, 1), 0.0)
    return jnp.concatenate([low, high], axis=1) * mask


def assemble(v_ref, ext_ref, xp_ref, c_ref, out):
    row = iota((NB, PL), 0)
    lane = iota((NB, 128), 1)

    def x_stage(t):
        for e in range(4):
            n = t * 4 + e
            m = v_ref[blk(n), :]
            if e > 0:
                left = v_ref[pl.ds(n * NB - 1, 1), :]
            else:
                left = ext_ref[pl.ds(t, 1), :]
            if e < 3:
                right = v_ref[pl.ds(n * NB + NB, 1), :]
            else:
                right = ext_ref[pl.ds(4 + t, 1), :]
            total = m + jnp.where(row == 0, left, 0.0) + jnp.where(row == NB - 1, right, 0.0)
            xp_ref[blk(n + 4), :] = total * c_ref[blk(n, C_ACT), :]

    def y_stage(t):
        for e in range(4):
            n = t * 4 + e
            x = xp_ref[blk(n + 4), :]
            before = xp_ref[blk(n), 128:]
            after = xp_ref[blk(n + 8), :128]
            low = x[:, :128] + jnp.where(lane < 16, pltpu.roll(before, 16, 1), 0.0)
            high = x[:, 128:] + jnp.where(lane >= 112, pltpu.roll(after, 112, 1), 0.0)
            z = jnp.concatenate([low, high], axis=1) * c_ref[blk(n, C_ACT), :]
            out(n, z)

    for t in range(4):
        x_stage(t)
    for t in range(4):
        y_stage(t)


def zero_borders(xp_ref):
    xp_ref[0:64, :] = jnp.zeros((64, PL), F32)
    xp_ref[320:384, :] = jnp.zeros((64, PL), F32)


def phase_one(step, c_ref, d_ref, bd_ref, wf_ref, wb_ref, s_in, s_out, v_ref, v2_ref, xp_ref, ext_ref,
              sm_ref, a_ref, b_ref):
    alpha, beta = step

    def forward(n):
        rows = blk(n)
        value = d_ref[blk(n, D_WGT), :] * s_out[blk(n, S_R), :]
        v2_ref[rows, :] = apply_weights(value, wf_ref, n)

    loop(16, forward, 8)
    for t in range(4):
        h = apply_blocks(bd_ref, 0, v2_ref[t * 64 : t * 64 + 64, :], t)
        h = h * d_ref[D_RD + t * 64 : D_RD + t * 64 + 64, :]
        v2_ref[t * 64 : t * 64 + 64, :] = apply_blocks(bd_ref, 1, h, t)

    def backward(n):
        v_ref[blk(n), :] = c_ref[blk(n, C_ACT), :] * apply_weights(v2_ref[blk(n), :], wb_ref, n)

    loop(16, backward, 8)
    ext_ref[...] = jnp.zeros((8, PL), F32)

    def update(n, z):
        new = beta * (d_ref[blk(n, D_WGT), :] * z)
        if alpha != 0.0:
            new = new + alpha * s_in[blk(n, S_U), :]
        s_out[blk(n, S_U), :] = new

    assemble(v_ref, ext_ref, xp_ref, c_ref, update)
    faces = [v_ref[t * 64 : t * 64 + 1, :] for t in range(4)]
    faces += [v_ref[t * 64 + 63 : t * 64 + 64, :] for t in range(4)]
    faces = jnp.concatenate(faces, axis=0)
    s_out[S_MF : S_MF + 8, :] = faces
    inner = []
    for side in range(2):
        for t in range(4):
            n = t * 4 + 3 * side
            k = c_ref[blk(side * 4 + t, C_KX), :]
            inner.append(jnp.sum(k * s_out[blk(n, S_U), :], axis=0, keepdims=True))
    inner = jnp.concatenate(inner, axis=0)
    to_left = jnp.concatenate([faces[:4], inner[:4]], axis=0)
    to_right = jnp.concatenate([faces[4:], inner[4:]], axis=0)
    even = jnp.full((8, PL), sm_ref[0], jnp.int32) == 0
    a_ref[...] = jnp.where(even, to_right, to_left)
    b_ref[...] = jnp.where(even, to_left, to_right)


def phase_two(step, c_ref, d_ref, bk_ref, m_ref, mg_ref, s_in, s_out, v_ref, v2_ref, xp_ref, ext_ref, sm_ref,
              a_ref, b_ref):
    alpha, beta = step
    even = jnp.full((8, PL), sm_ref[0], jnp.int32) == 0
    rec_a, rec_b = a_ref[...], b_ref[...]
    from_left = jnp.where(even, rec_b, rec_a)
    from_right = jnp.where(even, rec_a, rec_b)
    outer = jnp.concatenate([from_left[:4], from_right[:4]], axis=0)
    inner = jnp.concatenate([from_left[4:], from_right[4:]], axis=0)
    fact = d_ref[D_FACT : D_FACT + 8, :]
    gact = d_ref[D_GACT : D_GACT + 8, :]
    delta = beta * (d_ref[D_FW : D_FW + 8, :] * face_stage(fact * outer, fact))
    ghost = (outer + s_in[S_MF : S_MF + 8, :]) * gact
    ghost = beta * (d_ref[D_GW : D_GW + 8, :] * face_stage(ghost, gact))
    if alpha != 0.0:
        ghost = ghost + alpha * s_in[S_GU : S_GU + 8, :]
    s_out[S_GU : S_GU + 8, :] = ghost
    row = iota((NB, PL), 0)
    for t in range(4):
        for e in range(4):
            n = t * 4 + e
            u = s_in[blk(n, S_U), :]
            if e == 0:
                u = u + jnp.where(row == 0, delta[t : t + 1], 0.0)
            if e == 3:
                u = u + jnp.where(row == NB - 1, delta[4 + t : 5 + t], 0.0)
            s_out[blk(n, S_U), :] = u
            s_out[blk(n, S_X), :] = s_in[blk(n, S_X), :] + u

    for t in range(4):
        v2_ref[t * 64 : t * 64 + 64, :] = apply_blocks(
            bk_ref, 0, s_out[S_U + t * 64 : S_U + t * 64 + 64, :], t
        )
    high, low = split(ghost)
    both = jnp.concatenate([high, low], axis=0)
    row8 = iota((8, PL), 0)
    image = inner + d_ref[D_KGG : D_KGG + 8, :] * ghost
    for s in range(8):
        w = s
        part = dot(both, mg_ref[blk(2 * w, 0, PL), :])
        part = part[:8] + part[8:] + dot(high, mg_ref[blk(2 * w + 1, 0, PL), :])
        image = image + jnp.where(row8 == s, part, 0.0)
    ext_ref[...] = image * gact

    def local(n):
        rows = blk(n)
        q = v2_ref[rows, :] + apply_weights(s_out[blk(n, S_U), :], m_ref, n)
        v_ref[rows, :] = c_ref[blk(n, C_ACT), :] * q

    loop(16, local, 8)

    def update(n, z):
        s_out[blk(n, S_R), :] = s_in[blk(n, S_R), :] - z

    assemble(v_ref, ext_ref, xp_ref, c_ref, update)


OWN = [(t, e) for t in range(4) for e in range(4)]


def hot(condition):
    return jnp.where(condition, 1.0, 0.0).astype(BF16)


def hots():
    l, m = iota((PL, PL), 0), iota((PL, PL), 1)
    return (l, m, hot(l % NB == m // NB), hot(l % NB == m % NB), hot(l // NB == m // NB),
            hot(l // NB == m % NB))


def expand(p_ref, rows, mask, onehot):
    for i, row in enumerate(rows):
        p_ref[blk(i), :] = jnp.where(mask, row, 0.0)
    for start in range(0, len(rows) * NB, 128):
        high, low = split(p_ref[start : start + 128, :])
        yield start, dot(high, onehot) + dot(low, onehot)


def block_rows(bd_ref, which, parts):
    block = (iota((128, PL), 0) // NB) % 4 == iota((128, PL), 1) // NB
    for start, part in parts:
        high, low = split(jnp.where(block, part, 0.0))
        bd_ref[which * 512 + start : which * 512 + start + 128, :] = high
        bd_ref[which * 512 + 256 + start : which * 512 + 256 + start + 128, :] = low


def store_pair(w_ref, n, j, value):
    high, low = split(value)
    w_ref[pl.ds(pl.multiple_of(n * 512 + j * NB, 16), NB), :] = high
    w_ref[pl.ds(pl.multiple_of(n * 512 + 256 + j * NB, 16), NB), :] = low


def build_sums(m_ref, count, ta_ref, tb_ref):
    lane = iota((NB, PL), 1)
    by_col = lane % NB == iota((NB, PL), 0)

    def build(n):
        ty = ta_ref[blk(n), :]
        tz = tb_ref[blk(n), :]
        for j in range(NB):
            value = jnp.where(by_col, ty[j : j + 1, :], 0.0)
            store_pair(m_ref, n, j, value + jnp.where(lane // NB == j, tz, 0.0))

    loop(count, build, 2)


def along(index, order):
    return jnp.where((index.astype(F32) < order) | (index == NB - 1), 1.0, 0.0)


def side_stack(pick):
    return jnp.concatenate([pick(0, t) for t in range(4)] + [pick(1, t) for t in range(4)], axis=0)


def edge_rows(ref, base):
    return side_stack(
        lambda side, t: ref[base + t * 64 + 63 * side : base + t * 64 + 63 * side + 1, :]
    )


def pack_kernel(ord_hbm, route_hbm, load_hbm, stiff_hbm, table_hbm, eig_hbm, o_ref,
                ord_ref, route_ref, load_ref, stiff_ref, table_ref, eig_ref, sems):
    copies = [
        pltpu.make_async_copy(src, dst, sems.at[i])
        for i, (src, dst) in enumerate(
            ((load_hbm, load_ref), (stiff_hbm, stiff_ref), (table_hbm, table_ref),
             (eig_hbm, eig_ref), (ord_hbm, ord_ref), (route_hbm, route_ref))
        )
    ]
    for copy in copies:
        copy.start()
    lane = iota((1, PL), 1)
    for d in range(4):
        o_ref[d, 92:96, :] = jnp.zeros((4, PL), F32)
    for copy in copies:
        copy.wait()
    for d in range(4):
        o_ref[d, 0:64, :] = load_ref[...]
    for e in range(4):
        order = jnp.full((1, PL), ord_ref[e], jnp.int32).astype(F32)
        slot = jnp.full((1, PL), lax.rem(route_ref[e], 4), jnp.int32).astype(F32)
        tail = jnp.where(lane == 48, order, jnp.where(lane == 49, slot, 0.0))
        for d in range(4):
            for k in range(3):
                r = 3 * e + k
                o_ref[d, G_STIFF + r : G_STIFF + r + 1, :] = stiff_ref[e : e + 1, k * PL : (k + 1) * PL]
                o_ref[d, G_TABLE + r : G_TABLE + r + 1, :] = table_ref[e : e + 1, k * PL : (k + 1) * PL]
            o_ref[d, G_EIG + e : G_EIG + e + 1, :] = tail
            o_ref[d, G_EIG + e : G_EIG + e + 1, 0:48] = eig_ref[e : e + 1, :]


def pick_kernel(sm_ref, g_ref, a_ref, b_ref, t2_ref, t3_ref, l_ref, r_ref):
    for t in range(4):
        base = t * F_STEP
        for ref, e in ((l_ref, 0), (r_ref, 3)):
            face = e * NB + (NB - 1 if e else 0)
            slot = 1 if e == 0 else 0
            ref[base + F_TABLE : base + F_TABLE + 3, :] = g_ref[t, G_TABLE + 3 * slot : G_TABLE + 3 * slot + 3, :]
            ref[base + F_EIG : base + F_EIG + 1, :] = g_ref[t, G_EIG + slot : G_EIG + slot + 1, :]
            ref[base + F_FACE : base + F_FACE + 1, :] = g_ref[t, face : face + 1, :]
            ref[base + F_STIFF : base + F_STIFF + 3, :] = g_ref[t, G_STIFF + 3 * e : G_STIFF + 3 * e + 3, :]
            ref[base + F_ORDER : base + F_ORDER + 1, :] = g_ref[t, G_EIG + e : G_EIG + e + 1, :]
        for ref, slot in ((t2_ref, 2), (t3_ref, 3)):
            ref[4 * t : 4 * t + 3, :] = g_ref[t, G_TABLE + 3 * slot : G_TABLE + 3 * slot + 3, :]
            ref[4 * t + 3 : 4 * t + 4, :] = g_ref[t, G_EIG + slot : G_EIG + slot + 1, :]
    l_ref[36:40, :] = jnp.zeros((4, PL), F32)
    r_ref[36:40, :] = jnp.zeros((4, PL), F32)
    even = jnp.full((F_ROWS, PL), sm_ref[0], jnp.int32) == 0
    to_left, to_right = l_ref[...], r_ref[...]
    a_ref[...] = jnp.where(even, to_right, to_left)
    b_ref[...] = jnp.where(even, to_left, to_right)


def slab_kernel(sm_ref, g_ref, c_ref, bk_ref, m_ref, p_ref, ta_ref, tb_ref):
    row = iota((NB, PL), 0)
    lane = iota((NB, PL), 1)
    l, _, _, e2, e3, e4 = hots()

    def stiff(d):
        return [g_ref[t, G_STIFF + 3 * e + d : G_STIFF + 3 * e + d + 1, :] for t, e in OWN]

    block_rows(bk_ref, 0, expand(p_ref, stiff(0), lane // NB == row, e2))
    eig = jnp.concatenate([g_ref[t, G_EIG : G_EIG + 4, :] for t in range(4)], axis=0)
    ints = eig.astype(BF16)
    orders = dot(ints, hot(l == 48))
    c_ref[C_SLOT : C_SLOT + 16, :] = dot(ints, hot(l == 49))
    for n, (t, e) in enumerate(OWN):
        order = orders[n : n + 1, :]
        act = along(row, order) * (along(lane // NB, order) * along(lane % NB, order))
        c_ref[blk(n, C_ACT), :] = act
        c_ref[blk(n, C_LOAD), :] = act * g_ref[t, e * NB : (e + 1) * NB, :]
    for side in range(2):
        for t in range(4):
            e = 3 * side
            kx = g_ref[t, G_STIFF + 3 * e : G_STIFF + 3 * e + 1, :]
            edge = NB - 1 if side else 0
            col = jnp.sum(
                jnp.where((lane == edge * NB + row) & (row != edge), kx, 0.0), axis=1, keepdims=True
            )
            c_ref[blk(side * 4 + t, C_KX), :] = jnp.broadcast_to(col, (NB, PL))
    for start, part in expand(p_ref, stiff(1), lane % NB == row, e3):
        ta_ref[start : start + 128, :] = part
    for start, part in expand(p_ref, stiff(2), lane % NB == row, e4):
        tb_ref[start : start + 128, :] = part
    build_sums(m_ref, 16, ta_ref, tb_ref)


def first_kernel(sm_ref, g_ref, ra_ref, rb_ref, t2_ref, t3_ref, c_ref, m_ref, d_ref, bd_ref, wf_ref, wb_ref, mg_ref, s_ref, a_ref,
                 b_ref, v_ref, v2_ref, xp_ref, ext_ref, p_ref, ta_ref, tb_ref, h_ref, f_ref):
    even = jnp.full((F_ROWS, PL), sm_ref[0], jnp.int32) == 0
    rec_a, rec_b = ra_ref[...], rb_ref[...]
    f_ref[0] = jnp.where(even, rec_b, rec_a)
    f_ref[1] = jnp.where(even, rec_a, rec_b)
    zero_borders(xp_ref)
    row = iota((NB, PL), 0)
    lane = iota((NB, PL), 1)
    by_row = lane // NB == row
    by_col = lane % NB == row
    l, m, e1, e2, e3, e4 = hots()
    lane8 = iota((8, PL), 1)
    row8 = iota((8, PL), 0)

    for n, (t, e) in enumerate(OWN):
        slot = c_ref[C_SLOT + n : C_SLOT + n + 1, :]
        found = jnp.where(
            slot == 0.0,
            jnp.concatenate([g_ref[t, G_TABLE : G_TABLE + 3, :], g_ref[t, G_EIG : G_EIG + 1, :]], axis=0),
            0.0,
        )
        others = (
            f_ref[1, t * F_STEP : t * F_STEP + 4, :],
            t2_ref[4 * t : 4 * t + 4, :],
            t3_ref[4 * t : 4 * t + 4, :],
        )
        for g in range(3):
            found = jnp.where(slot == float(g + 1), others[g], found)
        h_ref[n * 8 : n * 8 + 4, :] = found

    def basis(d):
        return [h_ref[n * 8 + d : n * 8 + d + 1, :] for n in range(16)]

    block_rows(bd_ref, 0, expand(p_ref, basis(0), by_col, e4))
    block_rows(bd_ref, 1, expand(p_ref, basis(0), by_row, e2))
    eig = jnp.concatenate(basis(3), axis=0)
    high, low = split(eig)
    cross_hot = hot(l == 16 + m // NB) + hot(l == 32 + m % NB)
    cross = dot(high, cross_hot) + dot(low, cross_hot)
    for start, part in expand(p_ref, basis(3), lane == row, hot(l < 16)):
        v_ref[start : start + 128, :] = part
    for n in range(16):
        d_ref[blk(n, D_RD), :] = 1.0 / (v_ref[blk(n), :] + cross[n : n + 1, :])

    def ghost(r):
        return side_stack(
            lambda side, t: f_ref[side, t * F_STEP + r : t * F_STEP + r + 1, :]
        )

    there = jnp.where(row8 < 4, sm_ref[2], sm_ref[3]) > 0
    order = dot(ghost(F_ORDER).astype(BF16), hot(l == 48))
    gact = jnp.where(there, along(lane8 // NB, order) * along(lane8 % NB, order), 0.0)
    fact = edge_rows(c_ref, C_ACT)
    d_ref[D_FACT : D_FACT + 8, :] = fact
    d_ref[D_GACT : D_GACT + 8, :] = gact
    ghost_shares = face_stage((gact + fact) * gact, gact)
    d_ref[D_GW : D_GW + 8, :] = gact / jnp.maximum(ghost_shares, 1.0)
    pick = lane8 == jnp.where(row8 < 4, PL - 1, 0)
    kgg = jnp.sum(jnp.where(pick, ghost(F_STIFF), 0.0), axis=1, keepdims=True)
    d_ref[D_KGG : D_KGG + 8, :] = jnp.broadcast_to(kgg, (8, PL))

    v_ref[...] = c_ref[C_ACT : C_ACT + 256, :]
    ext_ref[...] = gact

    def weigh(n, z):
        d_ref[blk(n, D_WGT), :] = c_ref[blk(n, C_ACT), :] / jnp.maximum(z, 1.0)

    assemble(v_ref, ext_ref, xp_ref, c_ref, weigh)
    d_ref[D_FW : D_FW + 8, :] = edge_rows(d_ref, D_WGT)
    v_ref[...] = c_ref[C_LOAD : C_LOAD + 256, :]
    ext_ref[...] = gact * ghost(F_FACE)

    def start_residual(n, z):
        s_ref[blk(n, S_R), :] = z

    assemble(v_ref, ext_ref, xp_ref, c_ref, start_residual)
    s_ref[S_X : S_X + 256, :] = jnp.zeros((256, PL), F32)
    s_ref[S_GU : S_GU + 8, :] = jnp.zeros((8, PL), F32)

    def product(w_ref, mask, hot_y, hot_z):
        for start, part in expand(p_ref, basis(1), mask, hot_y):
            ta_ref[start : start + 128, :] = part
        for start, part in expand(p_ref, basis(2), mask, hot_z):
            tb_ref[start : start + 128, :] = part

        def build(n):
            ty = ta_ref[blk(n), :]
            tz = tb_ref[blk(n), :]
            for b in range(NB):
                store_pair(w_ref, n, b, ty[b : b + 1, :] * tz)

        loop(16, build, 2)

    product(wf_ref, by_row, e1, e2)
    product(wb_ref, by_col, e3, e4)

    def ghost_list(r):
        return [f_ref[side, t * F_STEP + r : t * F_STEP + r + 1, :]
                for side in range(2) for t in range(4)]

    for start, part in expand(p_ref, ghost_list(F_STIFF + 1), by_col, e3):
        ta_ref[start : start + 128, :] = part
    for start, part in expand(p_ref, ghost_list(F_STIFF + 2), by_col, e4):
        tb_ref[start : start + 128, :] = part
    build_sums(mg_ref, 8, ta_ref, tb_ref)
    phase_one(STEPS[0], c_ref, d_ref, bd_ref, wf_ref, wb_ref, s_ref, s_ref, v_ref, v2_ref, xp_ref,
              ext_ref, sm_ref, a_ref, b_ref)


def middle_kernel(k, sm_ref, ra_ref, rb_ref, c_ref, d_ref, bd_ref, bk_ref, wf_ref, wb_ref, m_ref,
                  mg_ref, si_ref, so_ref, a_ref, b_ref, v_ref, v2_ref, xp_ref, ext_ref):
    zero_borders(xp_ref)
    phase_two(STEPS[k], c_ref, d_ref, bk_ref, m_ref, mg_ref, si_ref, so_ref, v_ref, v2_ref, xp_ref,
              ext_ref, sm_ref, ra_ref, rb_ref)
    phase_one(STEPS[k + 1], c_ref, d_ref, bd_ref, wf_ref, wb_ref, so_ref, so_ref, v_ref, v2_ref,
              xp_ref, ext_ref, sm_ref, a_ref, b_ref)


def last_kernel(sm_ref, ra_ref, rb_ref, c_ref, d_ref, bk_ref, m_ref, mg_ref, si_ref, x_ref, r_ref,
                so_ref, v_ref, v2_ref, xp_ref, ext_ref):
    zero_borders(xp_ref)
    phase_two(STEPS[3], c_ref, d_ref, bk_ref, m_ref, mg_ref, si_ref, so_ref, v_ref, v2_ref, xp_ref,
              ext_ref, sm_ref, ra_ref, rb_ref)
    base = pl.multiple_of(sm_ref[1] * 64, 64)
    x_ref[...] = so_ref[pl.ds(S_X + base, 64), :]
    r_ref[...] = so_ref[pl.ds(S_R + base, 64), :]


VM = pl.BlockSpec(memory_space=pltpu.VMEM)
SM = pl.BlockSpec(memory_space=pltpu.SMEM)


def struct(rows, dtype=F32):
    return jax.ShapeDtypeStruct((rows, PL), dtype)


WORK = [pltpu.VMEM((256, PL), F32), pltpu.VMEM((256, PL), F32), pltpu.VMEM((384, PL), F32),
        pltpu.VMEM((8, PL), F32)]
LIMIT = pltpu.CompilerParams(vmem_limit_bytes=12 * 2**20)


def call(kernel, scalars, ins, outs, scratch=(), flops=2 * 10**9, where=VM):
    return pl.pallas_call(
        kernel,
        in_specs=[SM] * scalars + [where] * ins,
        out_specs=[VM] * len(outs),
        out_shape=outs,
        scratch_shapes=list(scratch),
        compiler_params=LIMIT,
        cost_estimate=pl.CostEstimate(flops=flops, transcendentals=0, bytes_accessed=2**20),
    )


def per_device(load_field, orders, stiffness, basis_table, eigen_values, route_plan):
    slabs = lax.axis_size("slab")
    tiles = lax.axis_size("tile")
    p = lax.axis_index("slab")
    tile = lax.axis_index("tile")
    scalars = jnp.stack([p % 2, tile, p, slabs - 1 - p]).astype(jnp.int32)
    swap_a = [(i, i ^ 1) for i in range(slabs)]
    swap_b = [(i, i + 1 if i % 2 else i - 1) for i in range(1, slabs - 1)]
    ring_b = [(i, (i + 1 if i % 2 else i - 1) % slabs) for i in range(slabs)]

    def gather(block):
        return lax.all_to_all(block, "tile", 0, 0)

    def ahead(block, distance):
        return lax.ppermute(block, "slab", [((i + distance) % slabs, i) for i in range(slabs)])

    (packed,) = call(
        pack_kernel, 0, 6, [jax.ShapeDtypeStruct((tiles, G_ROWS, PL), F32)],
        [pltpu.SMEM((4,), jnp.int32), pltpu.SMEM((4,), jnp.int32), pltpu.VMEM((64, PL), F32),
         pltpu.VMEM((4, 768), F32), pltpu.VMEM((4, 768), F32), pltpu.VMEM((4, 48), F32),
         pltpu.SemaphoreType.DMA((6,))],
        where=pl.BlockSpec(memory_space=pltpu.HBM),
    )(*[pltpu.with_memory_space_constraint(item, pltpu.HBM) for item in (
        orders, route_plan, load_field.reshape(64, PL), stiffness, basis_table, eigen_values)])
    slab = gather(packed)
    pa, pb, p2, p3 = call(
        pick_kernel, 1, 1, [struct(F_ROWS), struct(F_ROWS), struct(16), struct(16)],
        [pltpu.VMEM((F_ROWS, PL), F32)] * 2,
    )(scalars, slab)
    wide = pltpu.VMEM((256, PL), F32)
    rb = lax.ppermute(pb, "slab", ring_b)
    t3 = ahead(p3, 3)
    t2 = ahead(p2, 2)
    ra = lax.ppermute(pa, "slab", swap_a)
    consts, blocks_k, w_m = call(
        slab_kernel, 1, 1, [struct(C_ROWS), struct(512, BF16), struct(16 * 512, BF16)],
        [wide] * 3,
    )(scalars, slab)

    def exchange(a, b):
        rb = lax.ppermute(b, "slab", swap_b)
        ra = lax.ppermute(a, "slab", swap_a)
        return ra, rb

    message = struct(8)
    more, blocks, w_f, w_b, w_g, s, a, b = call(
        first_kernel,
        1,
        7,
        [struct(D_ROWS), struct(1024, BF16), struct(16 * 512, BF16), struct(16 * 512, BF16),
         struct(8 * 512, BF16), struct(S_ROWS), message, message],
        WORK + [wide] * 3 + [pltpu.VMEM((128, PL), F32), pltpu.VMEM((2, F_ROWS, PL), F32)],
    )(scalars, slab, ra, rb, t2, t3, consts, w_m)
    for k in range(3):
        ra, rb = exchange(a, b)

        def kernel(*refs, k=k):
            middle_kernel(k, *refs)

        s, a, b = call(
            kernel, 1, 11, [struct(S_ROWS), message, message], WORK
        )(scalars, ra, rb, consts, more, blocks, blocks_k, w_f, w_b, w_m, w_g, s)
    ra, rb = exchange(a, b)
    x, r = call(
        last_kernel, 1, 8, [struct(64), struct(64)],
        [pltpu.VMEM((S_ROWS, PL), F32)] + WORK,
    )(scalars, ra, rb, consts, more, blocks_k, w_m, w_g, s)
    return x.reshape(load_field.shape), r.reshape(load_field.shape)


def solution(mesh):
    both = ("slab", "tile")
    in_specs = (P(both, None, None), P(both), P(both, None), P(both, None), P(both, None), P(both))
    out_specs = (P(both, None, None), P(both, None, None))
    return jax.shard_map(
        per_device, mesh=mesh, in_specs=in_specs, out_specs=out_specs, check_vma=False
    )
```

```python
import jax
import jax.numpy as jnp
from jax import lax
from jax.experimental import pallas as pl
from jax.experimental.pallas import tpu as pltpu
from jax.sharding import PartitionSpec as P


F32 = jnp.float32
BF16 = jnp.bfloat16
NB = 16
PL = 256
CHEB_LOW, CHEB_HIGH = 0.4, 8.0
CENTER = (CHEB_HIGH + CHEB_LOW) / 2.0
HALF = (CHEB_HIGH - CHEB_LOW) / 2.0
SIGMA = CENTER / HALF
RATIO = 1.0 / SIGMA
RATIO_NEXT = 1.0 / (2.0 * SIGMA - RATIO)
STEPS = (
    (0.0, 1.0 / CENTER),
    (RATIO_NEXT * RATIO, 2.0 * RATIO_NEXT / HALF),
) * 2

G_STIFF, G_TABLE, G_EIG, G_ROWS = 64, 76, 88, 96
F_TABLE, F_EIG, F_FACE, F_STIFF, F_ORDER, F_STEP, F_ROWS = 0, 3, 4, 5, 8, 9, 40
C_ACT, C_KX, C_LOAD, C_SLOT, C_ROWS = 0, 256, 384, 640, 656
D_WGT, D_RD, D_FACT, D_GACT, D_FW, D_GW, D_KGG, D_ROWS = 0, 256, 512, 520, 528, 536, 544, 552
S_R, S_U, S_X, S_MF, S_GU, S_ROWS = 0, 256, 512, 768, 776, 784


def iota(shape, dim):
    return lax.broadcasted_iota(jnp.int32, shape, dim)


def split(value):
    high = value.astype(BF16)
    low = (value - high.astype(F32)).astype(BF16)
    return high, low


def dot(a, b):
    return jnp.dot(a, b, preferred_element_type=F32)


def blk(n, base=0, size=NB):
    if isinstance(n, int):
        return slice(base + n * size, base + (n + 1) * size)
    return pl.ds(pl.multiple_of(base + n * size, 8), size)


def loop(count, body, unroll):
    if unroll >= count:
        for k in range(count):
            body(k)
        return

    def step(i, carry):
        for k in range(unroll):
            body(i * unroll + k)
        return carry

    lax.fori_loop(0, count // unroll, step, 0)


def apply_weights(value, w_ref, n):
    rows = value.shape[0]
    high, low = split(value)
    both = dot(jnp.concatenate([high, low], axis=0), w_ref[blk(2 * n, 0, PL), :])
    return both[:rows] + both[rows:] + dot(high, w_ref[blk(2 * n + 1, 0, PL), :])


def apply_blocks(bd_ref, which, value, t):
    high, low = split(value)
    m_high = bd_ref[which * 512 + t * 64 : which * 512 + (t + 1) * 64, :64]
    m_low = bd_ref[which * 512 + 256 + t * 64 : which * 512 + 256 + (t + 1) * 64, :64]
    both = dot(jnp.concatenate([m_high, m_low], axis=0), high)
    return both[:64] + both[64:] + dot(m_high, low)


def face_stage(value, mask):
    low, high = value[:, :128], value[:, 128:]
    row = iota((8, 128), 0)
    lane = iota((8, 128), 1)
    before = jnp.where(row % 4 == 0, 0.0, pltpu.roll(high, 1, 0))
    after = jnp.where(row % 4 == 3, 0.0, pltpu.roll(low, 7, 0))
    low = low + jnp.where(lane < 16, pltpu.roll(before, 16, 1), 0.0)
    high = high + jnp.where(lane >= 112, pltpu.roll(after, 112, 1), 0.0)
    return jnp.concatenate([low, high], axis=1) * mask


def assemble(v_ref, ext_ref, xp_ref, c_ref, out):
    row = iota((NB, PL), 0)
    lane = iota((NB, 128), 1)

    def x_stage(t):
        for e in range(4):
            n = t * 4 + e
            m = v_ref[blk(n), :]
            if e > 0:
                left = v_ref[pl.ds(n * NB - 1, 1), :]
            else:
                left = ext_ref[pl.ds(t, 1), :]
            if e < 3:
                right = v_ref[pl.ds(n * NB + NB, 1), :]
            else:
                right = ext_ref[pl.ds(4 + t, 1), :]
            total = m + jnp.where(row == 0, left, 0.0) + jnp.where(row == NB - 1, right, 0.0)
            xp_ref[blk(n + 4), :] = total * c_ref[blk(n, C_ACT), :]

    def y_stage(t):
        for e in range(4):
            n = t * 4 + e
            x = xp_ref[blk(n + 4), :]
            before = xp_ref[blk(n), 128:]
            after = xp_ref[blk(n + 8), :128]
            low = x[:, :128] + jnp.where(lane < 16, pltpu.roll(before, 16, 1), 0.0)
            high = x[:, 128:] + jnp.where(lane >= 112, pltpu.roll(after, 112, 1), 0.0)
            z = jnp.concatenate([low, high], axis=1) * c_ref[blk(n, C_ACT), :]
            out(n, z)

    for t in range(4):
        x_stage(t)
    for t in range(4):
        y_stage(t)


def zero_borders(xp_ref):
    xp_ref[0:64, :] = jnp.zeros((64, PL), F32)
    xp_ref[320:384, :] = jnp.zeros((64, PL), F32)


def phase_one(step, c_ref, d_ref, bd_ref, wf_ref, wb_ref, s_in, s_out, v_ref, v2_ref, xp_ref, ext_ref,
              sm_ref, a_ref, b_ref, beside=(), unroll=16):
    alpha, beta = step

    def forward(n):
        rows = blk(n)
        value = d_ref[blk(n, D_WGT), :] * s_out[blk(n, S_R), :]
        v2_ref[rows, :] = apply_weights(value, wf_ref, n)
        for work in beside[:1]:
            work(n)

    loop(16, forward, unroll)
    for t in range(4):
        h = apply_blocks(bd_ref, 0, v2_ref[t * 64 : t * 64 + 64, :], t)
        h = h * d_ref[D_RD + t * 64 : D_RD + t * 64 + 64, :]
        v2_ref[t * 64 : t * 64 + 64, :] = apply_blocks(bd_ref, 1, h, t)

    def backward(n):
        v_ref[blk(n), :] = c_ref[blk(n, C_ACT), :] * apply_weights(v2_ref[blk(n), :], wb_ref, n)

    loop(16, backward, unroll)
    ext_ref[...] = jnp.zeros((8, PL), F32)

    def update(n, z):
        new = beta * (d_ref[blk(n, D_WGT), :] * z)
        if alpha != 0.0:
            new = new + alpha * s_in[blk(n, S_U), :]
        s_out[blk(n, S_U), :] = new

    assemble(v_ref, ext_ref, xp_ref, c_ref, update)
    faces = [v_ref[t * 64 : t * 64 + 1, :] for t in range(4)]
    faces += [v_ref[t * 64 + 63 : t * 64 + 64, :] for t in range(4)]
    faces = jnp.concatenate(faces, axis=0)
    s_out[S_MF : S_MF + 8, :] = faces
    inner = []
    for side in range(2):
        for t in range(4):
            n = t * 4 + 3 * side
            k = c_ref[blk(side * 4 + t, C_KX), :]
            inner.append(jnp.sum(k * s_out[blk(n, S_U), :], axis=0, keepdims=True))
    inner = jnp.concatenate(inner, axis=0)
    to_left = jnp.concatenate([faces[:4], inner[:4]], axis=0)
    to_right = jnp.concatenate([faces[4:], inner[4:]], axis=0)
    even = jnp.full((8, PL), sm_ref[0], jnp.int32) == 0
    a_ref[...] = jnp.where(even, to_right, to_left)
    b_ref[...] = jnp.where(even, to_left, to_right)


def phase_two(step, c_ref, d_ref, bk_ref, m_ref, mg_ref, s_in, s_out, v_ref, v2_ref, xp_ref, ext_ref, sm_ref,
              a_ref, b_ref):
    alpha, beta = step
    even = jnp.full((8, PL), sm_ref[0], jnp.int32) == 0
    rec_a, rec_b = a_ref[...], b_ref[...]
    from_left = jnp.where(even, rec_b, rec_a)
    from_right = jnp.where(even, rec_a, rec_b)
    outer = jnp.concatenate([from_left[:4], from_right[:4]], axis=0)
    inner = jnp.concatenate([from_left[4:], from_right[4:]], axis=0)
    fact = d_ref[D_FACT : D_FACT + 8, :]
    gact = d_ref[D_GACT : D_GACT + 8, :]
    delta = beta * (d_ref[D_FW : D_FW + 8, :] * face_stage(fact * outer, fact))
    ghost = (outer + s_in[S_MF : S_MF + 8, :]) * gact
    ghost = beta * (d_ref[D_GW : D_GW + 8, :] * face_stage(ghost, gact))
    if alpha != 0.0:
        ghost = ghost + alpha * s_in[S_GU : S_GU + 8, :]
    s_out[S_GU : S_GU + 8, :] = ghost
    row = iota((NB, PL), 0)
    for t in range(4):
        for e in range(4):
            n = t * 4 + e
            u = s_in[blk(n, S_U), :]
            if e == 0:
                u = u + jnp.where(row == 0, delta[t : t + 1], 0.0)
            if e == 3:
                u = u + jnp.where(row == NB - 1, delta[4 + t : 5 + t], 0.0)
            s_out[blk(n, S_U), :] = u
            s_out[blk(n, S_X), :] = s_in[blk(n, S_X), :] + u

    for t in range(4):
        v2_ref[t * 64 : t * 64 + 64, :] = apply_blocks(
            bk_ref, 0, s_out[S_U + t * 64 : S_U + t * 64 + 64, :], t
        )
    high, low = split(ghost)
    both = jnp.concatenate([high, low], axis=0)
    row8 = iota((8, PL), 0)
    image = inner + d_ref[D_KGG : D_KGG + 8, :] * ghost
    for s in range(8):
        w = s
        part = dot(both, mg_ref[blk(2 * w, 0, PL), :])
        part = part[:8] + part[8:] + dot(high, mg_ref[blk(2 * w + 1, 0, PL), :])
        image = image + jnp.where(row8 == s, part, 0.0)
    ext_ref[...] = image * gact

    def local(n):
        rows = blk(n)
        q = v2_ref[rows, :] + apply_weights(s_out[blk(n, S_U), :], m_ref, n)
        v_ref[rows, :] = c_ref[blk(n, C_ACT), :] * q

    loop(16, local, 16)

    def update(n, z):
        s_out[blk(n, S_R), :] = s_in[blk(n, S_R), :] - z

    assemble(v_ref, ext_ref, xp_ref, c_ref, update)


OWN = [(t, e) for t in range(4) for e in range(4)]


def hot(condition):
    return jnp.where(condition, 1.0, 0.0).astype(BF16)


def hots():
    l, m = iota((PL, PL), 0), iota((PL, PL), 1)
    return (l, m, hot(l % NB == m // NB), hot(l % NB == m % NB), hot(l // NB == m // NB),
            hot(l // NB == m % NB))


def expand(p_ref, rows, mask, onehot):
    for i, row in enumerate(rows):
        p_ref[blk(i), :] = jnp.where(mask, row, 0.0)
    for start in range(0, len(rows) * NB, 128):
        high, low = split(p_ref[start : start + 128, :])
        yield start, dot(high, onehot) + dot(low, onehot)


def block_rows(bd_ref, which, parts):
    block = (iota((128, PL), 0) // NB) % 4 == iota((128, PL), 1) // NB
    for start, part in parts:
        high, low = split(jnp.where(block, part, 0.0))
        bd_ref[which * 512 + start : which * 512 + start + 128, :] = high
        bd_ref[which * 512 + 256 + start : which * 512 + 256 + start + 128, :] = low


def store_pair(w_ref, n, j, value):
    high, low = split(value)
    w_ref[blk(n * 32 + j), :] = high
    w_ref[blk(n * 32 + 16 + j), :] = low


def build_sums(m_ref, count, ta_ref, tb_ref):
    lane = iota((NB, PL), 1)
    by_col = lane % NB == iota((NB, PL), 0)

    def build(n):
        ty = ta_ref[blk(n), :]
        tz = tb_ref[blk(n), :]
        for j in range(NB):
            value = jnp.where(by_col, ty[j : j + 1, :], 0.0)
            store_pair(m_ref, n, j, value + jnp.where(lane // NB == j, tz, 0.0))

    loop(count, build, 2)


def along(index, order):
    return jnp.where((index.astype(F32) < order) | (index == NB - 1), 1.0, 0.0)


def side_stack(pick):
    return jnp.concatenate([pick(0, t) for t in range(4)] + [pick(1, t) for t in range(4)], axis=0)


def edge_rows(ref, base):
    return side_stack(
        lambda side, t: ref[base + t * 64 + 63 * side : base + t * 64 + 63 * side + 1, :]
    )


def pack_kernel(ord_hbm, route_hbm, load_hbm, stiff_hbm, table_hbm, eig_hbm, o_ref,
                ord_ref, route_ref, load_ref, stiff_ref, table_ref, eig_ref, sems):
    copies = [
        pltpu.make_async_copy(src, dst, sems.at[i])
        for i, (src, dst) in enumerate(
            ((load_hbm, load_ref), (stiff_hbm, stiff_ref), (table_hbm, table_ref),
             (eig_hbm, eig_ref), (ord_hbm, ord_ref), (route_hbm, route_ref))
        )
    ]
    for copy in copies:
        copy.start()
    lane = iota((1, PL), 1)
    for d in range(4):
        o_ref[d, 92:96, :] = jnp.zeros((4, PL), F32)
    for copy in copies:
        copy.wait()
    for d in range(4):
        o_ref[d, 0:64, :] = load_ref[...]
    for e in range(4):
        order = jnp.full((1, PL), ord_ref[e], jnp.int32).astype(F32)
        slot = jnp.full((1, PL), lax.rem(route_ref[e], 4), jnp.int32).astype(F32)
        tail = jnp.where(lane == 48, order, jnp.where(lane == 49, slot, 0.0))
        for d in range(4):
            for k in range(3):
                r = 3 * e + k
                o_ref[d, G_STIFF + r : G_STIFF + r + 1, :] = stiff_ref[e : e + 1, k * PL : (k + 1) * PL]
                o_ref[d, G_TABLE + r : G_TABLE + r + 1, :] = table_ref[e : e + 1, k * PL : (k + 1) * PL]
            o_ref[d, G_EIG + e : G_EIG + e + 1, :] = tail
            o_ref[d, G_EIG + e : G_EIG + e + 1, 0:48] = eig_ref[e : e + 1, :]


def pick_kernel(sm_ref, g_ref, a_ref, b_ref, t2_ref, t3_ref, l_ref, r_ref):
    for t in range(4):
        base = t * F_STEP
        for ref, e in ((l_ref, 0), (r_ref, 3)):
            face = e * NB + (NB - 1 if e else 0)
            slot = 1 if e == 0 else 0
            ref[base + F_TABLE : base + F_TABLE + 3, :] = g_ref[t, G_TABLE + 3 * slot : G_TABLE + 3 * slot + 3, :]
            ref[base + F_EIG : base + F_EIG + 1, :] = g_ref[t, G_EIG + slot : G_EIG + slot + 1, :]
            ref[base + F_FACE : base + F_FACE + 1, :] = g_ref[t, face : face + 1, :]
            ref[base + F_STIFF : base + F_STIFF + 3, :] = g_ref[t, G_STIFF + 3 * e : G_STIFF + 3 * e + 3, :]
            ref[base + F_ORDER : base + F_ORDER + 1, :] = g_ref[t, G_EIG + e : G_EIG + e + 1, :]
        for ref, slot in ((t2_ref, 2), (t3_ref, 3)):
            ref[4 * t : 4 * t + 3, :] = g_ref[t, G_TABLE + 3 * slot : G_TABLE + 3 * slot + 3, :]
            ref[4 * t + 3 : 4 * t + 4, :] = g_ref[t, G_EIG + slot : G_EIG + slot + 1, :]
    l_ref[36:40, :] = jnp.zeros((4, PL), F32)
    r_ref[36:40, :] = jnp.zeros((4, PL), F32)
    even = jnp.full((F_ROWS, PL), sm_ref[0], jnp.int32) == 0
    to_left, to_right = l_ref[...], r_ref[...]
    a_ref[...] = jnp.where(even, to_right, to_left)
    b_ref[...] = jnp.where(even, to_left, to_right)


def slab_kernel(sm_ref, g_ref, c_ref, bk_ref, m_ref, p_ref, ta_ref, tb_ref):
    row = iota((NB, PL), 0)
    lane = iota((NB, PL), 1)
    l, _, _, e2, e3, e4 = hots()

    def stiff(d):
        return [g_ref[t, G_STIFF + 3 * e + d : G_STIFF + 3 * e + d + 1, :] for t, e in OWN]

    block_rows(bk_ref, 0, expand(p_ref, stiff(0), lane // NB == row, e2))
    eig = jnp.concatenate([g_ref[t, G_EIG : G_EIG + 4, :] for t in range(4)], axis=0)
    ints = eig.astype(BF16)
    orders = dot(ints, hot(l == 48))
    c_ref[C_SLOT : C_SLOT + 16, :] = dot(ints, hot(l == 49))
    for n, (t, e) in enumerate(OWN):
        order = orders[n : n + 1, :]
        act = along(row, order) * (along(lane // NB, order) * along(lane % NB, order))
        c_ref[blk(n, C_ACT), :] = act
        c_ref[blk(n, C_LOAD), :] = act * g_ref[t, e * NB : (e + 1) * NB, :]
    for side in range(2):
        for t in range(4):
            e = 3 * side
            kx = g_ref[t, G_STIFF + 3 * e : G_STIFF + 3 * e + 1, :]
            edge = NB - 1 if side else 0
            col = jnp.sum(
                jnp.where((lane == edge * NB + row) & (row != edge), kx, 0.0), axis=1, keepdims=True
            )
            c_ref[blk(side * 4 + t, C_KX), :] = jnp.broadcast_to(col, (NB, PL))
    for start, part in expand(p_ref, stiff(1), lane % NB == row, e3):
        ta_ref[start : start + 128, :] = part
    for start, part in expand(p_ref, stiff(2), lane % NB == row, e4):
        tb_ref[start : start + 128, :] = part
    build_sums(m_ref, 16, ta_ref, tb_ref)


def first_kernel(sm_ref, g_ref, ra_ref, rb_ref, t2_ref, t3_ref, c_ref, m_ref, d_ref, bd_ref, wf_ref, wb_ref, mg_ref, s_ref, a_ref,
                 b_ref, v_ref, v2_ref, xp_ref, ext_ref, p_ref, ta_ref, tb_ref, h_ref, f_ref, tc_ref,
                 td_ref):
    even = jnp.full((F_ROWS, PL), sm_ref[0], jnp.int32) == 0
    rec_a, rec_b = ra_ref[...], rb_ref[...]
    f_ref[0] = jnp.where(even, rec_b, rec_a)
    f_ref[1] = jnp.where(even, rec_a, rec_b)
    zero_borders(xp_ref)
    row = iota((NB, PL), 0)
    lane = iota((NB, PL), 1)
    by_row = lane // NB == row
    by_col = lane % NB == row
    l, m, e1, e2, e3, e4 = hots()
    lane8 = iota((8, PL), 1)
    row8 = iota((8, PL), 0)

    for n, (t, e) in enumerate(OWN):
        slot = c_ref[C_SLOT + n : C_SLOT + n + 1, :]
        found = jnp.where(
            slot == 0.0,
            jnp.concatenate([g_ref[t, G_TABLE : G_TABLE + 3, :], g_ref[t, G_EIG : G_EIG + 1, :]], axis=0),
            0.0,
        )
        others = (
            f_ref[1, t * F_STEP : t * F_STEP + 4, :],
            t2_ref[4 * t : 4 * t + 4, :],
            t3_ref[4 * t : 4 * t + 4, :],
        )
        for g in range(3):
            found = jnp.where(slot == float(g + 1), others[g], found)
        h_ref[n * 8 : n * 8 + 4, :] = found

    def basis(d):
        return [h_ref[n * 8 + d : n * 8 + d + 1, :] for n in range(16)]

    block_rows(bd_ref, 0, expand(p_ref, basis(0), by_col, e4))
    block_rows(bd_ref, 1, expand(p_ref, basis(0), by_row, e2))
    eig = jnp.concatenate(basis(3), axis=0)
    high, low = split(eig)
    cross_hot = hot(l == 16 + m // NB) + hot(l == 32 + m % NB)
    cross = dot(high, cross_hot) + dot(low, cross_hot)
    for start, part in expand(p_ref, basis(3), lane == row, hot(l < 16)):
        v_ref[start : start + 128, :] = part
    for n in range(16):
        d_ref[blk(n, D_RD), :] = 1.0 / (v_ref[blk(n), :] + cross[n : n + 1, :])

    def ghost(r):
        return side_stack(
            lambda side, t: f_ref[side, t * F_STEP + r : t * F_STEP + r + 1, :]
        )

    there = jnp.where(row8 < 4, sm_ref[2], sm_ref[3]) > 0
    order = dot(ghost(F_ORDER).astype(BF16), hot(l == 48))
    gact = jnp.where(there, along(lane8 // NB, order) * along(lane8 % NB, order), 0.0)
    fact = edge_rows(c_ref, C_ACT)
    d_ref[D_FACT : D_FACT + 8, :] = fact
    d_ref[D_GACT : D_GACT + 8, :] = gact
    ghost_shares = face_stage((gact + fact) * gact, gact)
    d_ref[D_GW : D_GW + 8, :] = gact / jnp.maximum(ghost_shares, 1.0)
    pick = lane8 == jnp.where(row8 < 4, PL - 1, 0)
    kgg = jnp.sum(jnp.where(pick, ghost(F_STIFF), 0.0), axis=1, keepdims=True)
    d_ref[D_KGG : D_KGG + 8, :] = jnp.broadcast_to(kgg, (8, PL))

    v_ref[...] = c_ref[C_ACT : C_ACT + 256, :]
    ext_ref[...] = gact

    def weigh(n, z):
        d_ref[blk(n, D_WGT), :] = c_ref[blk(n, C_ACT), :] / jnp.maximum(z, 1.0)

    assemble(v_ref, ext_ref, xp_ref, c_ref, weigh)
    d_ref[D_FW : D_FW + 8, :] = edge_rows(d_ref, D_WGT)
    v_ref[...] = c_ref[C_LOAD : C_LOAD + 256, :]
    ext_ref[...] = gact * ghost(F_FACE)

    def start_residual(n, z):
        s_ref[blk(n, S_R), :] = z

    assemble(v_ref, ext_ref, xp_ref, c_ref, start_residual)
    s_ref[S_X : S_X + 256, :] = jnp.zeros((256, PL), F32)
    s_ref[S_GU : S_GU + 8, :] = jnp.zeros((8, PL), F32)

    def product(w_ref, y_ref, z_ref, mask, hot_y, hot_z):
        for start, part in expand(p_ref, basis(1), mask, hot_y):
            y_ref[start : start + 128, :] = part
        for start, part in expand(p_ref, basis(2), mask, hot_z):
            z_ref[start : start + 128, :] = part

        def build(n):
            ty = y_ref[blk(n), :]
            tz = z_ref[blk(n), :]
            for b in range(NB):
                store_pair(w_ref, n, b, ty[b : b + 1, :] * tz)

        return build

    loop(16, product(wf_ref, ta_ref, tb_ref, by_row, e1, e2), 2)
    build_second = product(wb_ref, tc_ref, td_ref, by_col, e3, e4)

    def ghost_list(r):
        return [f_ref[side, t * F_STEP + r : t * F_STEP + r + 1, :]
                for side in range(2) for t in range(4)]

    for start, part in expand(p_ref, ghost_list(F_STIFF + 1), by_col, e3):
        ta_ref[start : start + 128, :] = part
    for start, part in expand(p_ref, ghost_list(F_STIFF + 2), by_col, e4):
        tb_ref[start : start + 128, :] = part
    build_sums(mg_ref, 8, ta_ref, tb_ref)
    phase_one(STEPS[0], c_ref, d_ref, bd_ref, wf_ref, wb_ref, s_ref, s_ref, v_ref, v2_ref, xp_ref,
              ext_ref, sm_ref, a_ref, b_ref, beside=(build_second,))


def middle_kernel(k, sm_ref, ra_ref, rb_ref, c_ref, d_ref, bd_ref, bk_ref, wf_ref, wb_ref, m_ref,
                  mg_ref, si_ref, so_ref, a_ref, b_ref, v_ref, v2_ref, xp_ref, ext_ref):
    zero_borders(xp_ref)
    phase_two(STEPS[k], c_ref, d_ref, bk_ref, m_ref, mg_ref, si_ref, so_ref, v_ref, v2_ref, xp_ref,
              ext_ref, sm_ref, ra_ref, rb_ref)
    phase_one(STEPS[k + 1], c_ref, d_ref, bd_ref, wf_ref, wb_ref, so_ref, so_ref, v_ref, v2_ref,
              xp_ref, ext_ref, sm_ref, a_ref, b_ref)


def last_kernel(sm_ref, ra_ref, rb_ref, c_ref, d_ref, bk_ref, m_ref, mg_ref, si_ref, x_ref, r_ref,
                so_ref, v_ref, v2_ref, xp_ref, ext_ref):
    zero_borders(xp_ref)
    phase_two(STEPS[3], c_ref, d_ref, bk_ref, m_ref, mg_ref, si_ref, so_ref, v_ref, v2_ref, xp_ref,
              ext_ref, sm_ref, ra_ref, rb_ref)
    base = pl.multiple_of(sm_ref[1] * 64, 64)
    x_ref[...] = so_ref[pl.ds(S_X + base, 64), :]
    r_ref[...] = so_ref[pl.ds(S_R + base, 64), :]


VM = pl.BlockSpec(memory_space=pltpu.VMEM)
SM = pl.BlockSpec(memory_space=pltpu.SMEM)


def struct(rows, dtype=F32):
    return jax.ShapeDtypeStruct((rows, PL), dtype)


WORK = [pltpu.VMEM((256, PL), F32), pltpu.VMEM((256, PL), F32), pltpu.VMEM((384, PL), F32),
        pltpu.VMEM((8, PL), F32)]
LIMIT = pltpu.CompilerParams(vmem_limit_bytes=12 * 2**20)


def call(kernel, scalars, ins, outs, scratch=(), flops=2 * 10**9, where=VM):
    return pl.pallas_call(
        kernel,
        in_specs=[SM] * scalars + [where] * ins,
        out_specs=[VM] * len(outs),
        out_shape=outs,
        scratch_shapes=list(scratch),
        compiler_params=LIMIT,
        cost_estimate=pl.CostEstimate(flops=flops, transcendentals=0, bytes_accessed=2**20),
    )


def per_device(load_field, orders, stiffness, basis_table, eigen_values, route_plan):
    slabs = lax.axis_size("slab")
    tiles = lax.axis_size("tile")
    p = lax.axis_index("slab")
    tile = lax.axis_index("tile")
    scalars = jnp.stack([p % 2, tile, p, slabs - 1 - p]).astype(jnp.int32)
    swap_a = [(i, i ^ 1) for i in range(slabs)]
    swap_b = [(i, i + 1 if i % 2 else i - 1) for i in range(1, slabs - 1)]
    ring_b = [(i, (i + 1 if i % 2 else i - 1) % slabs) for i in range(slabs)]

    def gather(block):
        return lax.all_to_all(block, "tile", 0, 0)

    def ahead(block, distance):
        return lax.ppermute(block, "slab", [((i + distance) % slabs, i) for i in range(slabs)])

    (packed,) = call(
        pack_kernel, 0, 6, [jax.ShapeDtypeStruct((tiles, G_ROWS, PL), F32)],
        [pltpu.SMEM((4,), jnp.int32), pltpu.SMEM((4,), jnp.int32), pltpu.VMEM((64, PL), F32),
         pltpu.VMEM((4, 768), F32), pltpu.VMEM((4, 768), F32), pltpu.VMEM((4, 48), F32),
         pltpu.SemaphoreType.DMA((6,))],
        where=pl.BlockSpec(memory_space=pltpu.HBM),
    )(*[pltpu.with_memory_space_constraint(item, pltpu.HBM) for item in (
        orders, route_plan, load_field.reshape(64, PL), stiffness, basis_table, eigen_values)])
    slab = gather(packed)
    pa, pb, p2, p3 = call(
        pick_kernel, 1, 1, [struct(F_ROWS), struct(F_ROWS), struct(16), struct(16)],
        [pltpu.VMEM((F_ROWS, PL), F32)] * 2,
    )(scalars, slab)
    wide = pltpu.VMEM((256, PL), F32)
    rb = lax.ppermute(pb, "slab", ring_b)
    t3 = ahead(p3, 3)
    t2 = ahead(p2, 2)
    ra = lax.ppermute(pa, "slab", swap_a)
    consts, blocks_k, w_m = call(
        slab_kernel, 1, 1, [struct(C_ROWS), struct(512, BF16), struct(16 * 512, BF16)],
        [wide] * 3,
    )(scalars, slab)

    def exchange(a, b):
        rb = lax.ppermute(b, "slab", swap_b)
        ra = lax.ppermute(a, "slab", swap_a)
        return ra, rb

    message = struct(8)
    more, blocks, w_f, w_b, w_g, s, a, b = call(
        first_kernel,
        1,
        7,
        [struct(D_ROWS), struct(1024, BF16), struct(16 * 512, BF16), struct(16 * 512, BF16),
         struct(8 * 512, BF16), struct(S_ROWS), message, message],
        WORK + [wide] * 3 + [pltpu.VMEM((128, PL), F32), pltpu.VMEM((2, F_ROWS, PL), F32), wide, wide],
    )(scalars, slab, ra, rb, t2, t3, consts, w_m)
    for k in range(3):
        ra, rb = exchange(a, b)

        def kernel(*refs, k=k):
            middle_kernel(k, *refs)

        s, a, b = call(
            kernel, 1, 11, [struct(S_ROWS), message, message], WORK
        )(scalars, ra, rb, consts, more, blocks, blocks_k, w_f, w_b, w_m, w_g, s)
    ra, rb = exchange(a, b)
    x, r = call(
        last_kernel, 1, 8, [struct(64), struct(64)],
        [pltpu.VMEM((S_ROWS, PL), F32)] + WORK,
    )(scalars, ra, rb, consts, more, blocks_k, w_m, w_g, s)
    return x.reshape(load_field.shape), r.reshape(load_field.shape)


def solution(mesh):
    both = ("slab", "tile")
    in_specs = (P(both, None, None), P(both), P(both, None), P(both, None), P(both, None), P(both))
    out_specs = (P(both, None, None), P(both, None, None))
    return jax.shard_map(
        per_device, mesh=mesh, in_specs=in_specs, out_specs=out_specs, check_vma=False
    )
```
